32 devices in a mesh: grp: 2 (over y), kvp: 4 (over x, core), tp: 4 (over z).
Axes of the slice: x: 2, y: 2, z: 4, core: 2. Of those that a mesh axis runs over, the one named last changes fastest.
Arguments:
- normed: bfloat16 [512, 6144], P('grp', 'kvp'), parts along dimension 0, may hold values from -6 to 6
- w_query: bfloat16 [6144, 6144], P('kvp', 'tp'), may hold values from -0.078125 to 0.078125
- w_key: bfloat16 [6144, 1024], P('kvp', 'tp'), may hold values from -0.078125 to 0.078125
- w_value: bfloat16 [6144, 1024], P('kvp', 'tp'), may hold values from -0.078125 to 0.078125
- w_out: bfloat16 [6144, 6144], P('tp', 'kvp'), may hold values from -0.078125 to 0.078125
- key_cache: bfloat16 [8, 1024, 128, 128], P('tp', ('grp', 'kvp')), parts along dimension 1, may hold values from -128 to 128
- value_cache: bfloat16 [8, 1024, 128, 128], P('tp', ('grp', 'kvp')), parts along dimension 1, may hold values from -6 to 6
- lengths: int32 [512], P('grp'), parts along dimension 0, may hold values from 1 to 12288, as said below
- page_table: int32 [512, 96], P('grp'), parts along dimension 0, may hold values from -1 to 511, as said below
Outputs:
- attended: bfloat16 [512, 6144], P(('grp', 'tp'), 'kvp'), parts along dimension 0
The draws below stay inside these ranges and needn't reach their ends.
There are 2 independent parts, one for each index of `grp`. The reference program is written for one: setup_inputs(seed, part) draws one part's arguments, and reference() takes and returns one part's arrays. A program takes and returns all parts, laid end to end along the dimension named above; an argument that names none is the same for every part. Nothing has to cross between parts.
Inputs may be any that keep to these rules, and one draw needn't show every extreme that they name: `lengths`: every request has at least one cached token; the longest request fills all 96 entries of its page table. `page_table`: entry [b, j] is a page index exactly when j < ceil(lengths[b] / 128), else -1; no page is named twice. Index kvp = i holds pages i * 128 to (i + 1) * 128 - 1; the pages in use are spread unevenly over kvp.
All inputs are finite; a program needn't handle non-finite values.
Results may differ from the reference program's by a relative error of at most 0.012.
Values may be sent and summed in bfloat16 or wider, within the bound.
A program may use at most 64 MiB of HBM per device.

```python
import jax
import jax.numpy as jnp
from jax import lax

D = 6144
HEADS = 48
KV_HEADS = 8
HEAD_DIM = 128
BATCH = 256
PAGES_DEV = 128
PAGE = 128
SLOTS = 512
USED = 384
MAXP = 96


def layout(key):
    base = jax.random.fold_in(key, 4242)
    keys = jax.random.split(base, 7)
    longest = jax.random.randint(keys[0], (), 0, BATCH)
    rows = jnp.arange(BATCH, dtype=jnp.int32)
    raw = jax.random.randint(keys[1], (BATCH,), 1, 65) * jax.random.randint(keys[2], (BATCH,), 1, 65)
    raw = jnp.where(rows == longest, 0, raw)
    spare = USED - MAXP - (BATCH - 1)
    extra = raw * spare // jnp.maximum(jnp.sum(raw), 1)
    blocks = jnp.minimum(1 + extra, MAXP)
    blocks = jnp.where(rows == longest, MAXP, blocks)
    tail = jax.random.randint(keys[3], (BATCH,), 1, PAGE + 1)
    lengths = (blocks - 1) * PAGE + tail
    lengths = jnp.where(rows == longest, MAXP * PAGE, lengths).astype(jnp.int32)
    pages = jnp.arange(SLOTS, dtype=jnp.int32)
    device = pages // PAGES_DEV
    within = pages % PAGES_DEV
    devices = SLOTS // PAGES_DEV
    bias = jax.random.randint(keys[4], (devices,), 1, 5)[device]
    tie = jax.random.permutation(keys[5], SLOTS).astype(jnp.int32)
    score = within * bias * SLOTS + tie
    order = jnp.argsort(score, stable=True).astype(jnp.int32)
    chosen = order[:USED]
    chosen = chosen[jax.random.permutation(keys[6], USED)]
    offsets = jnp.cumsum(blocks) - blocks
    column = jnp.arange(MAXP, dtype=jnp.int32)
    flat = offsets[:, None] + column[None, :]
    valid = column[None, :] < blocks[:, None]
    table = jnp.where(valid, chosen[jnp.clip(flat, 0, USED - 1)], -1).astype(jnp.int32)
    return (lengths, table)


def draw_lengths(key, part):
    return layout(key)[0]


def draw_page_table(key, part):
    return layout(key)[1]


def draw_key_cache(key, part):
    first = jax.random.fold_in(jax.random.fold_in(key, 77), 0)
    values = jnp.clip(jax.random.normal(first, (KV_HEADS, SLOTS, PAGE, HEAD_DIM), jnp.float32), -4.0, 4.0)
    return values.astype(jnp.bfloat16)


def levels(rng, shape, cuts, smallest, top_value):
    def one(dim, shards_of):
        heights = jax.random.uniform(jax.random.fold_in(jax.random.fold_in(rng, 6), dim), (shards_of,), jnp.float32, smallest / len(cuts), top_value / len(cuts))
        return jnp.repeat(jnp.exp(heights), shape[dim] // shards_of).reshape((-1,) + (1,) * (len(shape) - dim - 1))

    factor_of = one(*cuts[0])
    for cut in cuts[1:]:
        factor_of = factor_of * one(*cut)
    return factor_of


def normal_values(stream_key, dims, spread, limit, cuts=(), held_as=jnp.bfloat16):
    array = spread * jax.random.normal(stream_key, dims, jnp.float32)
    if cuts:
        array = array * levels(stream_key, dims, cuts, -0.22, 0.18)
    return jnp.clip(array, -limit, limit).astype(held_as)


def setup_inputs(seed: int = 0, part: int = 0) -> dict:
    arg_keys = jax.random.split(jax.random.key(seed), 10)
    part_keys = jax.random.split(jax.random.fold_in(arg_keys[9], part), 10)
    normed = normal_values(part_keys[0], (BATCH, D), 1.0, 6.0, ((1, 4),))
    w_query = normal_values(arg_keys[1], (D, HEADS * HEAD_DIM), D ** -0.5, 0.078125, ((0, 4), (1, 4)))
    w_key = normal_values(arg_keys[2], (D, KV_HEADS * HEAD_DIM), D ** -0.5, 0.078125, ((0, 4), (1, 4)))
    w_value = normal_values(arg_keys[3], (D, KV_HEADS * HEAD_DIM), D ** -0.5, 0.078125, ((0, 4), (1, 4)))
    w_out = normal_values(arg_keys[4], (HEADS * HEAD_DIM, D), (HEADS * HEAD_DIM) ** -0.5, 0.078125, ((0, 4), (1, 4)))
    key_cache = draw_key_cache(jax.random.fold_in(jax.random.fold_in(arg_keys[9], part), 71), part)
    value_cache = normal_values(part_keys[6], (KV_HEADS, SLOTS, PAGE, HEAD_DIM), 1.0, 6.0, ((0, 4), (1, 4)))
    lengths = draw_lengths(jax.random.fold_in(jax.random.fold_in(arg_keys[9], part), 71), part)
    page_table = draw_page_table(jax.random.fold_in(jax.random.fold_in(arg_keys[9], part), 71), part)
    return dict(normed=normed, w_query=w_query, w_key=w_key, w_value=w_value, w_out=w_out, key_cache=key_cache, value_cache=value_cache, lengths=lengths, page_table=page_table)


ROPE_BASE = 1000000.0
NEG = -1.0e30
TWO_PI_HIGH = 6.28125
TWO_PI_LOW = 0.0019353071795864769


def rotate(x, pos):
    width = x.shape[-1]
    half = width // 2
    freq = ROPE_BASE ** (-(2.0 * jnp.arange(half, dtype=jnp.float32)) / width)
    coarse = lax.optimization_barrier(freq.astype(jnp.bfloat16)).astype(jnp.float32)
    fine = freq - coarse
    pos_e = pos[..., None]
    exact = pos_e * coarse
    turns = jnp.floor(exact / TWO_PI_HIGH)
    angle = (exact - turns * TWO_PI_HIGH) - turns * TWO_PI_LOW + pos_e * fine
    cosine = jnp.cos(angle)
    sine = jnp.sin(angle)
    first = x[..., :half]
    second = x[..., half:]
    return jnp.concatenate([first * cosine - second * sine, second * cosine + first * sine], axis=-1)


def reference(normed, w_query, w_key, w_value, w_out, key_cache, value_cache, lengths, page_table):
    group = HEADS // KV_HEADS
    query = jnp.dot(normed, w_query, preferred_element_type=jnp.float32)
    key_new = jnp.dot(normed, w_key, preferred_element_type=jnp.float32)
    value_new = jnp.dot(normed, w_value, preferred_element_type=jnp.float32)
    position = lengths.astype(jnp.float32)
    q_rot = rotate(query.reshape(BATCH, KV_HEADS, group, HEAD_DIM), position[:, None, None]).astype(jnp.bfloat16)
    k_rot = rotate(key_new.reshape(BATCH, KV_HEADS, HEAD_DIM), position[:, None]).astype(jnp.bfloat16)
    v_new = value_new.reshape(BATCH, KV_HEADS, HEAD_DIM).astype(jnp.bfloat16)
    scale = HEAD_DIM ** -0.5

    def one_request(items):
        q_one, k_one, v_one, length, table = items
        index = jnp.maximum(table, 0).astype(jnp.int32)
        keys = key_cache[:, index].reshape(KV_HEADS, MAXP * PAGE, HEAD_DIM).astype(jnp.float32)
        values = value_cache[:, index].reshape(KV_HEADS, MAXP * PAGE, HEAD_DIM).astype(jnp.float32)
        valid = jnp.arange(MAXP * PAGE, dtype=jnp.int32) < length
        qf = q_one.astype(jnp.float32)
        scores = jnp.einsum('hgd,htd->hgt', qf, keys) * scale
        scores = jnp.where(valid[None, None, :], scores, NEG)
        s_new = jnp.einsum('hgd,hd->hg', qf, k_one.astype(jnp.float32)) * scale
        top = jnp.maximum(jnp.max(scores, axis=-1), s_new)
        weights = jnp.where(valid[None, None, :], jnp.exp(scores - top[..., None]), 0.0)
        w_new = jnp.exp(s_new - top)
        total = jnp.sum(weights, axis=-1) + w_new
        acc = jnp.einsum('hgt,htd->hgd', weights.astype(jnp.bfloat16).astype(jnp.float32), values)
        acc = acc + w_new[..., None] * v_one.astype(jnp.float32)[:, None, :]
        return (acc / total[..., None]).astype(jnp.bfloat16)

    head_out = lax.map(one_request, (q_rot, k_rot, v_new, lengths, page_table))
    head_out = head_out.reshape(BATCH, HEADS * HEAD_DIM)
    return jnp.dot(head_out, w_out, preferred_element_type=jnp.float32).astype(jnp.bfloat16)
```

```python
import functools

import jax
import jax.numpy as jnp
from jax import lax
from jax.experimental import pallas as pl
from jax.experimental.pallas import tpu as pltpu
from jax.sharding import PartitionSpec as P

ROPE_BASE = 1000000.0
NEG = -1e30
TWO_PI_HIGH = 6.28125
TWO_PI_LOW = 0.0019353071795864768
MESH = pl.DeviceIdType.MESH
VMEM_LIMIT = 60 * 1024 * 1024


def angles(pos, width):
    half = width // 2
    freq = ROPE_BASE ** (-(2.0 * jnp.arange(half, dtype=jnp.float32)) / width)
    coarse = lax.optimization_barrier(freq.astype(jnp.bfloat16)).astype(jnp.float32)
    fine = freq - coarse
    pos_e = pos[..., None]
    exact = pos_e * coarse
    turns = jnp.floor(exact / TWO_PI_HIGH)
    angle = exact - turns * TWO_PI_HIGH - turns * TWO_PI_LOW + pos_e * fine
    cosine = jnp.cos(angle)
    sine = jnp.sin(angle)
    return (
        jnp.concatenate([cosine, cosine], axis=-1),
        jnp.concatenate([-sine, sine], axis=-1),
    )


def chunks_of(count, most):
    size = most
    while count % size:
        size -= 1
    return [(start, size) for start in range(0, count, size)]


def place(m):
    me = lax.axis_index("kvp")
    core = me % 2
    chip = me // 2
    partner = chip * 2 + (1 - core)
    peers = [((chip + s) % m) * 2 + core for s in range(1, m)]
    return core, partner, peers


def remote(src, dst, send, recv, axis, index):
    return pltpu.make_async_remote_copy(
        src_ref=src, dst_ref=dst, send_sem=send, recv_sem=recv,
        device_id={axis: index}, device_id_type=MESH,
    )


def greet(devices):
    barrier = pltpu.get_barrier_semaphore()
    for axis, index in devices:
        pl.semaphore_signal(barrier, inc=1, device_id={axis: index}, device_id_type=MESH)
    pl.semaphore_wait(barrier, len(devices))


def project_kernel(
    m, x, wq, wk, wv, cos, sin, ptt,
    q_out, kv_out, mt_out,
    wbuf, own, s1, r1, s2, r2,
    wsem, ss1, rs1, ss2, rs2, ss3, rs3,
):
    nq = q_out.shape[0]
    nkv = kv_out.shape[0] // 2
    hd = q_out.shape[2]
    half = own.shape[1]
    core, partner, peers = place(m)
    parts = chunks_of(nq, 3) + [(nq, 2 * nkv)]
    count = len(parts)
    loads = []
    for i, (h0, n) in enumerate(parts):
        if i < count - 1:
            loads.append([pltpu.make_async_copy(
                wq.at[:, pl.ds(h0 * hd, n * hd)], wbuf.at[:, pl.ds(h0 * hd, n * hd)], wsem.at[i])])
        else:
            loads.append([
                pltpu.make_async_copy(wk, wbuf.at[:, pl.ds(nq * hd, nkv * hd)], wsem.at[i]),
                pltpu.make_async_copy(wv, wbuf.at[:, pl.ds((nq + nkv) * hd, nkv * hd)], wsem.at[i + 1]),
            ])
    for group in loads:
        for load in group:
            load.start()
    greet([("kvp", partner)] + [("kvp", p) for p in peers])
    mine = pl.ds(pl.multiple_of(core * half, half), half)
    other = pl.ds(pl.multiple_of((1 - core) * half, half), half)
    first, second, third = [], [], []

    def stage1(i):
        h0, n = parts[i]
        for load in loads[i]:
            load.wait()
        w = wbuf[:, h0 * hd:(h0 + n) * hd]
        theirs = jnp.dot(x[other, :], w, preferred_element_type=jnp.float32)
        for j in range(n):
            s1[h0 + j] = theirs[:, j * hd:(j + 1) * hd].astype(jnp.bfloat16)
        copy = remote(s1.at[pl.ds(h0, n)], r1.at[pl.ds(h0, n)], ss1.at[i], rs1.at[i], "kvp", partner)
        copy.start()
        first.append(copy)
        ours = jnp.dot(x[mine, :], w, preferred_element_type=jnp.float32)
        for j in range(n):
            own[h0 + j] = ours[:, j * hd:(j + 1) * hd]

    def stage2(i):
        h0, n = parts[i]
        first[i].wait_recv()
        for h in range(h0, h0 + n):
            value = own[h] + r1[h].astype(jnp.float32)
            own[h] = value
            s2[h] = value.astype(jnp.bfloat16)
        group = []
        for s, peer in enumerate(peers):
            copy = remote(
                s2.at[pl.ds(h0, n)], r2.at[s, pl.ds(h0, n)], ss2.at[s, i], rs2.at[s, i], "kvp", peer)
            copy.start()
            group.append(copy)
        second.append(group)

    for i in range(count):
        stage1(i)
        if i:
            stage2(i - 1)
    stage2(count - 1)

    slots, batch = mt_out.shape
    base = lax.axis_index("kvp") * slots
    ids = lax.broadcasted_iota(jnp.int32, (slots, batch), 0) + base

    def mark(j, found):
        row = ptt[pl.ds(j, 1), :]
        return jnp.where(row == ids, j, found)

    mt_out[...] = lax.fori_loop(
        0, ptt.shape[0], mark, jnp.full((slots, batch), -1, jnp.int32), unroll=4)

    cosine = cos[mine, :]
    sine = sin[mine, :]

    def turn(value):
        return (value * cosine + pltpu.roll(value, hd // 2, 1) * sine).astype(jnp.bfloat16)

    for i in range(count):
        h0, n = parts[i]
        for copy in second[i]:
            copy.wait_recv()
        for h in range(h0, h0 + n):
            value = own[h]
            for s in range(len(peers)):
                value = value + r2[s, h].astype(jnp.float32)
            if h < nq:
                q_out[h, mine, :] = turn(value)
            elif h < nq + nkv:
                kv_out[h - nq] = turn(value)
            else:
                kv_out[h - nq] = value.astype(jnp.bfloat16)
        if i < count - 1:
            part = q_out.at[pl.ds(h0, n), mine, :]
            copy = remote(part, part, ss3.at[i], rs3.at[i], "kvp", partner)
            copy.start()
            third.append(copy)
    for copy in first:
        copy.wait_send()
    for group in second:
        for copy in group:
            copy.wait_send()
    for copy in third:
        copy.wait()


def project(m, x, wq, wk, wv, cos, sin, ptt, slots, hd):
    batch, depth = x.shape
    nq = wq.shape[1] // hd
    nkv = wk.shape[1] // hd
    heads = nq + 2 * nkv
    half = batch // 2
    nqc = len(chunks_of(nq, 3))
    vmem = pl.BlockSpec(memory_space=pltpu.VMEM)
    hbm = pl.BlockSpec(memory_space=pl.ANY)
    dma = pltpu.SemaphoreType.DMA
    return pl.pallas_call(
        functools.partial(project_kernel, m),
        out_shape=(
            jax.ShapeDtypeStruct((nq, batch, hd), jnp.bfloat16),
            jax.ShapeDtypeStruct((2 * nkv, half, hd), jnp.bfloat16),
            jax.ShapeDtypeStruct((slots, batch), jnp.int32),
        ),
        in_specs=[vmem, hbm, hbm, hbm, vmem, vmem, vmem],
        out_specs=(vmem, vmem, vmem),
        scratch_shapes=[
            pltpu.VMEM((depth, heads * hd), jnp.bfloat16),
            pltpu.VMEM((heads, half, hd), jnp.float32),
            pltpu.VMEM((heads, half, hd), jnp.bfloat16),
            pltpu.VMEM((heads, half, hd), jnp.bfloat16),
            pltpu.VMEM((heads, half, hd), jnp.bfloat16),
            pltpu.VMEM((m - 1, heads, half, hd), jnp.bfloat16),
            dma((nqc + 2,)), dma((nqc + 1,)), dma((nqc + 1,)),
            dma((m - 1, nqc + 1)), dma((m - 1, nqc + 1)), dma((nqc,)), dma((nqc,)),
        ],
        compiler_params=pltpu.CompilerParams(
            collective_id=0, has_side_effects=True, vmem_limit_bytes=VMEM_LIMIT),
    )(x, wq, wk, wv, cos, sin, ptt)


def finish_kernel(
    m, ntp, o, stats, q, kv, wout, out,
    wbuf, r1o, r1s, mo, s2o, s2s, r2o, r2s, tile, ho, snew, tsend, town, trecv,
    wsem, s1sem, r1sem, s2sem, r2sem, s3sem, r3sem, s4sem, r4sem,
):
    nq, half, hd = mo.shape
    nqp = stats.shape[1] // 2
    core, partner, peers = place(m)
    tp = lax.axis_index("tp")
    load = pltpu.make_async_copy(wout, wbuf, wsem)
    load.start()
    greet(
        [("kvp", partner)] + [("kvp", p) for p in peers]
        + [("tp", (tp + d) % ntp) for d in range(1, ntp)]
    )
    mine = pl.ds(pl.multiple_of(core * half, half), half)
    other = pl.ds(pl.multiple_of((1 - core) * half, half), half)
    parts = chunks_of(nq, 3)
    count = len(parts)
    stat1 = remote(stats.at[1 - core], r1s, s1sem.at[count], r1sem.at[count], "kvp", partner)
    stat1.start()
    first = []
    for i, (h0, n) in enumerate(parts):
        copy = remote(
            o.at[pl.ds(h0, n), other, :], r1o.at[pl.ds(h0, n)], s1sem.at[i], r1sem.at[i], "kvp", partner)
        copy.start()
        first.append(copy)
    nkv = kv.shape[0] // 2
    group = nq // nkv
    ones = jnp.ones((8, hd), jnp.float32)
    snew[...] = jnp.full(snew.shape, NEG, jnp.float32)
    for h in range(nq):
        product = q[h, mine, :].astype(jnp.float32) * kv[h // group].astype(jnp.float32)
        row = lax.dot_general(
            ones, product, (((1,), (1,)), ((), ())),
            precision=lax.Precision.HIGHEST, preferred_element_type=jnp.float32)
        snew[h:h + 1, :] = row[0:1] * (hd ** -0.5)

    def merged(sources):
        top = sources[0][0]
        for t, _ in sources[1:]:
            top = jnp.maximum(top, t)
        raw = [jnp.exp(t - top) * total for t, total in sources]
        total = raw[0]
        for r in raw[1:]:
            total = total + r
        safe = jnp.where(total > 0.0, total, 1.0)
        for k, r in enumerate(raw):
            tile[k * nqp:(k + 1) * nqp, :] = r / safe
        return top, total, tile[...].T

    tile[...] = jnp.zeros(tile.shape, jnp.float32)
    stat1.wait_recv()
    top, total, cols = merged([
        (stats[core, :nqp], stats[core, nqp:]), (r1s[:nqp], r1s[nqp:]),
    ])
    s2s[:nqp] = top
    s2s[nqp:] = total
    stat2 = []
    for s, peer in enumerate(peers):
        copy = remote(s2s, r2s.at[s], s2sem.at[s, count], r2sem.at[s, count], "kvp", peer)
        copy.start()
        stat2.append(copy)
    second = []
    for i, (h0, n) in enumerate(parts):
        first[i].wait_recv()
        for h in range(h0, h0 + n):
            value = (
                cols[:, h:h + 1] * o[h, mine, :].astype(jnp.float32)
                + cols[:, nqp + h:nqp + h + 1] * r1o[h].astype(jnp.float32)
            )
            mo[h] = value
            s2o[h] = value.astype(jnp.bfloat16)
        copies = []
        for s, peer in enumerate(peers):
            copy = remote(
                s2o.at[pl.ds(h0, n)], r2o.at[s, pl.ds(h0, n)], s2sem.at[s, i], r2sem.at[s, i], "kvp", peer)
            copy.start()
            copies.append(copy)
        second.append(copies)
    for copy in stat2:
        copy.wait_recv()
    sources = [(top, total)]
    for s in range(len(peers)):
        sources.append((r2s[s, :nqp], r2s[s, nqp:]))
    sources.append((snew[...], jnp.ones(snew.shape, jnp.float32)))
    _, _, cols = merged(sources)
    last = len(sources) - 1
    third = []
    for i, (h0, n) in enumerate(parts):
        for copy in second[i]:
            copy.wait_recv()
        for h in range(h0, h0 + n):
            value = cols[:, h:h + 1] * mo[h]
            for s in range(len(peers)):
                at = (s + 1) * nqp + h
                value = value + cols[:, at:at + 1] * r2o[s, h].astype(jnp.float32)
            at = last * nqp + h
            value = value + cols[:, at:at + 1] * kv[nkv + h // group].astype(jnp.float32)
            ho[mine, h * hd:(h + 1) * hd] = value.astype(jnp.bfloat16)
        part = ho.at[mine, pl.ds(h0 * hd, n * hd)]
        copy = remote(part, part, s3sem.at[i], r3sem.at[i], "kvp", partner)
        copy.start()
        third.append(copy)
    load.wait()
    for copy in third:
        copy.wait()
    pieces, batch, width = tsend.shape
    rows = batch // ntp
    fourth = []
    keep = pl.ds(pl.multiple_of(tp * rows, rows), rows)
    for j in range(pieces):
        terms = jnp.dot(
            ho[...], wbuf[:, j * width:(j + 1) * width], preferred_element_type=jnp.float32)
        town[...] = terms
        tsend[j] = terms.astype(jnp.bfloat16)
        copies = []
        for d in range(1, ntp):
            to = (tp + d) % ntp
            take = pl.ds(pl.multiple_of(to * rows, rows), rows)
            copy = remote(
                tsend.at[j, take, :], trecv.at[d - 1, j], s4sem.at[d - 1, j], r4sem.at[d - 1, j], "tp", to)
            copy.start()
            copies.append(copy)
        fourth.append(copies)
        mo_piece = town[keep, :]
        wbuf_keep = pl.ds(j * width, width)
        out[:, wbuf_keep] = mo_piece
    for j in range(pieces):
        value = out[:, j * width:(j + 1) * width]
        for d in range(1, ntp):
            fourth[j][d - 1].wait_recv()
            value = value + trecv[d - 1, j].astype(jnp.float32)
        out[:, j * width:(j + 1) * width] = value
    stat1.wait_send()
    for copy in first + stat2:
        copy.wait_send()
    for copies in second + fourth:
        for copy in copies:
            copy.wait_send()


def finish(m, ntp, o, stats, q, kv, wout):
    nq, batch, hd = o.shape
    half = batch // 2
    nqp = stats.shape[1] // 2
    count = len(chunks_of(nq, 3))
    width = wout.shape[1]
    pieces = len(chunks_of(width // hd, 3))
    rows = batch // ntp
    tile_rows = max((m + 1) * nqp, half)
    vmem = pl.BlockSpec(memory_space=pltpu.VMEM)
    hbm = pl.BlockSpec(memory_space=pl.ANY)
    dma = pltpu.SemaphoreType.DMA
    return pl.pallas_call(
        functools.partial(finish_kernel, m, ntp),
        out_shape=jax.ShapeDtypeStruct((rows, width), jnp.float32),
        in_specs=[vmem, vmem, vmem, vmem, hbm],
        out_specs=vmem,
        scratch_shapes=[
            pltpu.VMEM(wout.shape, jnp.bfloat16),
            pltpu.VMEM((nq, half, hd), jnp.bfloat16),
            pltpu.VMEM((2 * nqp, half), jnp.float32),
            pltpu.VMEM((nq, half, hd), jnp.float32),
            pltpu.VMEM((nq, half, hd), jnp.bfloat16),
            pltpu.VMEM((2 * nqp, half), jnp.float32),
            pltpu.VMEM((m - 1, nq, half, hd), jnp.bfloat16),
            pltpu.VMEM((m - 1, 2 * nqp, half), jnp.float32),
            pltpu.VMEM((tile_rows, half), jnp.float32),
            pltpu.VMEM((batch, nq * hd), jnp.bfloat16),
            pltpu.VMEM((nqp, half), jnp.float32),
            pltpu.VMEM((pieces, batch, width // pieces), jnp.bfloat16),
            pltpu.VMEM((batch, width // pieces), jnp.float32),
            pltpu.VMEM((ntp - 1, pieces, rows, width // pieces), jnp.bfloat16),
            dma, dma((count + 1,)), dma((count + 1,)),
            dma((m - 1, count + 1)), dma((m - 1, count + 1)),
            dma((count,)), dma((count,)),
            dma((ntp - 1, pieces)), dma((ntp - 1, pieces)),
        ],
        compiler_params=pltpu.CompilerParams(
            collective_id=1, has_side_effects=True, vmem_limit_bytes=VMEM_LIMIT),
    )(o, stats, q, kv, wout)


def attend(q, mt, lengths, key_cache, value_cache):
    nq, batch, hd = q.shape
    nkv, slots, page, _ = key_cache.shape
    group = nq // nkv
    hit = mt >= 0
    held = jnp.sum(jnp.where(hit, lengths[None, :] - mt * page, 0), axis=1)
    valid = jnp.arange(page, dtype=jnp.int32)[None, :] < held[:, None]
    mask = valid[None, :, None, :]
    owned = jnp.einsum("pb,hbd->hpd", hit.astype(jnp.bfloat16), q)
    owned = owned.reshape(nkv, group, slots, hd)
    scores = jnp.einsum(
        "hgpd,hptd->hpgt", owned, key_cache, preferred_element_type=jnp.float32) * hd ** -0.5
    scores = jnp.where(mask, scores, NEG)
    slot_top = jnp.max(scores, axis=-1)
    weights = jnp.where(mask, jnp.exp(scores - slot_top[..., None]), 0.0)
    slot_total = jnp.sum(weights, axis=-1)
    slot_acc = jnp.einsum(
        "hpgt,hptd->hpgd", weights.astype(jnp.bfloat16), value_cache,
        preferred_element_type=jnp.float32)
    cover = hit[None, :, None, :]
    top = jnp.max(jnp.where(cover, slot_top[..., None], NEG), axis=1)
    factor = jnp.where(cover, jnp.exp(slot_top[..., None] - top[:, None]), 0.0)
    total = jnp.sum(factor * slot_total[..., None], axis=1)
    acc = jnp.einsum("hpgb,hpgd->hgbd", factor, slot_acc, preferred_element_type=jnp.float32)
    safe = jnp.where(total > 0.0, total, 1.0)
    o = (acc / safe[..., None]).astype(jnp.bfloat16).reshape(nq, batch, hd)
    nqp = -(-nq // 8) * 8
    pad = ((0, nqp - nq), (0, 0))
    stats = jnp.concatenate(
        [
            jnp.pad(top.reshape(nq, batch), pad, constant_values=NEG),
            jnp.pad(total.reshape(nq, batch), pad),
        ]
    )
    return o, stats.reshape(2 * nqp, 2, batch // 2).transpose(1, 0, 2)


def body(m, ntp, normed, w_query, w_key, w_value, w_out, key_cache, value_cache, lengths, page_table):
    hd = key_cache.shape[3]
    cos, sin = angles(lengths.astype(jnp.float32), hd)
    q, kv, mt = project(
        m, normed, w_query, w_key, w_value, cos, sin, page_table.T, key_cache.shape[1], hd)
    o, stats = attend(q, mt, lengths, key_cache, value_cache)
    return finish(m, ntp, o, stats, q, kv, w_out).astype(jnp.bfloat16)


def solution(mesh):
    return jax.shard_map(
        functools.partial(body, mesh.shape["kvp"] // 2, mesh.shape["tp"]),
        mesh=mesh,
        in_specs=(
            P("grp", "kvp"),
            P("kvp", "tp"),
            P("kvp", "tp"),
            P("kvp", "tp"),
            P("tp", "kvp"),
            P("tp", ("grp", "kvp"), None, None),
            P("tp", ("grp", "kvp"), None, None),
            P("grp"),
            P("grp", None),
        ),
        out_specs=P(("grp", "tp"), "kvp"),
        check_vma=False,
    )
```

```python
import functools

import jax
import jax.numpy as jnp
from jax import lax
from jax.experimental import pallas as pl
from jax.experimental.pallas import tpu as pltpu
from jax.sharding import PartitionSpec as P

ROPE_BASE = 1000000.0
NEG = -1e30
TWO_PI_HIGH = 6.28125
TWO_PI_LOW = 0.0019353071795864768
MESH = pl.DeviceIdType.MESH
VMEM_LIMIT = 60 * 1024 * 1024


def angles(pos, width):
    half = width // 2
    lane = jnp.arange(width, dtype=jnp.int32)
    freq = ROPE_BASE ** (-(2.0 * (lane % half).astype(jnp.float32)) / width)
    coarse = lax.optimization_barrier(freq.astype(jnp.bfloat16)).astype(jnp.float32)
    fine = freq - coarse
    pos_e = pos[..., None]
    exact = pos_e * coarse
    turns = jnp.floor(exact / TWO_PI_HIGH)
    angle = exact - turns * TWO_PI_HIGH - turns * TWO_PI_LOW + pos_e * fine
    sign = jnp.where(lane < half, -1.0, 1.0)
    return jnp.cos(angle), jnp.sin(angle) * sign


def chunks_of(count, most):
    size = most
    while count % size:
        size -= 1
    return [(start, size) for start in range(0, count, size)]


def place(m):
    me = lax.axis_index("kvp")
    core = me % 2
    chip = me // 2
    partner = chip * 2 + (1 - core)
    peers = [((chip + s) % m) * 2 + core for s in range(1, m)]
    return core, partner, peers


def remote(src, dst, send, recv, axis, index):
    return pltpu.make_async_remote_copy(
        src_ref=src, dst_ref=dst, send_sem=send, recv_sem=recv,
        device_id={axis: index}, device_id_type=MESH,
    )


def greet(devices):
    barrier = pltpu.get_barrier_semaphore()
    for axis, index in devices:
        pl.semaphore_signal(barrier, inc=1, device_id={axis: index}, device_id_type=MESH)
    pl.semaphore_wait(barrier, len(devices))


def project_kernel(
    m, x, wq, wk, wv, cos, sin, ptt, lens,
    q_out, kv_out, mt_out, owned_out, valid_out,
    wbuf, own, s1, r1, s2, r2,
    wsem, ss1, rs1, ss2, rs2, ss3, rs3,
):
    nq = q_out.shape[0]
    nkv = kv_out.shape[0] // 2
    hd = q_out.shape[2]
    half = own.shape[1]
    core, partner, peers = place(m)
    parts = chunks_of(nq, 3) + [(nq, 2 * nkv)]
    count = len(parts)
    loads = []
    for i, (h0, n) in enumerate(parts):
        if i < count - 1:
            loads.append([pltpu.make_async_copy(
                wq.at[:, pl.ds(h0 * hd, n * hd)], wbuf.at[:, pl.ds(h0 * hd, n * hd)], wsem.at[i])])
        else:
            loads.append([
                pltpu.make_async_copy(wk, wbuf.at[:, pl.ds(nq * hd, nkv * hd)], wsem.at[i]),
                pltpu.make_async_copy(wv, wbuf.at[:, pl.ds((nq + nkv) * hd, nkv * hd)], wsem.at[i + 1]),
            ])
    for group in loads:
        for load in group:
            load.start()
    greet([("kvp", partner)] + [("kvp", p) for p in peers])
    mine = pl.ds(pl.multiple_of(core * half, half), half)
    other = pl.ds(pl.multiple_of((1 - core) * half, half), half)
    first, second, third = [], [], []

    def stage1(i):
        h0, n = parts[i]
        for load in loads[i]:
            load.wait()
        w = wbuf[:, h0 * hd:(h0 + n) * hd]
        theirs = jnp.dot(x[other, :], w, preferred_element_type=jnp.float32)
        for j in range(n):
            s1[h0 + j] = theirs[:, j * hd:(j + 1) * hd].astype(jnp.bfloat16)
        copy = remote(s1.at[pl.ds(h0, n)], r1.at[pl.ds(h0, n)], ss1.at[i], rs1.at[i], "kvp", partner)
        copy.start()
        first.append(copy)
        ours = jnp.dot(x[mine, :], w, preferred_element_type=jnp.float32)
        for j in range(n):
            own[h0 + j] = ours[:, j * hd:(j + 1) * hd]

    def stage2(i):
        h0, n = parts[i]
        first[i].wait_recv()
        for h in range(h0, h0 + n):
            value = own[h] + r1[h].astype(jnp.float32)
            own[h] = value
            s2[h] = value.astype(jnp.bfloat16)
        group = []
        for s, peer in enumerate(peers):
            copy = remote(
                s2.at[pl.ds(h0, n)], r2.at[s, pl.ds(h0, n)], ss2.at[s, i], rs2.at[s, i], "kvp", peer)
            copy.start()
            group.append(copy)
        second.append(group)

    for i in range(count):
        stage1(i)
        if i:
            stage2(i - 1)
    stage2(count - 1)

    slots, batch = mt_out.shape
    base = lax.axis_index("kvp") * slots
    ids = lax.broadcasted_iota(jnp.int32, (slots, batch), 0) + base

    def mark(j, found):
        row = ptt[pl.ds(j, 1), :]
        return jnp.where(row == ids, j, found)

    found = lax.fori_loop(
        0, ptt.shape[0], mark, jnp.full((slots, batch), -1, jnp.int32), unroll=4)
    mt_out[...] = found
    page = valid_out.shape[1]
    left = jnp.where(found >= 0, lens[...] - found * page, 0)
    held = jnp.sum(left, axis=1, keepdims=True)
    token = lax.broadcasted_iota(jnp.int32, (slots, page), 1)
    valid_out[...] = jnp.where(token < held, 1, 0)
    hot = jnp.where(found >= 0, 1.0, 0.0).astype(jnp.bfloat16)

    cosine = cos[mine, :]
    sine = sin[mine, :]

    def turn(value):
        return (value * cosine + pltpu.roll(value, hd // 2, 1) * sine).astype(jnp.bfloat16)

    for i in range(count):
        h0, n = parts[i]
        for copy in second[i]:
            copy.wait_recv()
        for h in range(h0, h0 + n):
            value = own[h]
            for s in range(len(peers)):
                value = value + r2[s, h].astype(jnp.float32)
            if h < nq:
                q_out[h, mine, :] = turn(value)
            elif h < nq + nkv:
                kv_out[h - nq] = turn(value)
            else:
                kv_out[h - nq] = value.astype(jnp.bfloat16)
        if i < count - 1:
            part = q_out.at[pl.ds(h0, n), mine, :]
            copy = remote(part, part, ss3.at[i], rs3.at[i], "kvp", partner)
            copy.start()
            third.append(copy)
    for i, copy in enumerate(third):
        h0, n = parts[i]
        copy.wait_recv()
        for h in range(h0, h0 + n):
            owned_out[h] = jnp.dot(
                hot, q_out[h], preferred_element_type=jnp.float32).astype(jnp.bfloat16)
    for copy in first + third:
        copy.wait_send()
    for group in second:
        for copy in group:
            copy.wait_send()


def project(m, x, wq, wk, wv, cos, sin, ptt, lens, slots, page, hd):
    batch, depth = x.shape
    nq = wq.shape[1] // hd
    nkv = wk.shape[1] // hd
    heads = nq + 2 * nkv
    half = batch // 2
    nqc = len(chunks_of(nq, 3))
    vmem = pl.BlockSpec(memory_space=pltpu.VMEM)
    hbm = pl.BlockSpec(memory_space=pl.ANY)
    dma = pltpu.SemaphoreType.DMA
    return pl.pallas_call(
        functools.partial(project_kernel, m),
        out_shape=(
            jax.ShapeDtypeStruct((nq, batch, hd), jnp.bfloat16),
            jax.ShapeDtypeStruct((2 * nkv, half, hd), jnp.bfloat16),
            jax.ShapeDtypeStruct((slots, batch), jnp.int32),
            jax.ShapeDtypeStruct((nq, slots, hd), jnp.bfloat16),
            jax.ShapeDtypeStruct((slots, page), jnp.int32),
        ),
        in_specs=[vmem, hbm, hbm, hbm, vmem, vmem, vmem, vmem],
        out_specs=(vmem,) * 5,
        scratch_shapes=[
            pltpu.VMEM((depth, heads * hd), jnp.bfloat16),
            pltpu.VMEM((heads, half, hd), jnp.float32),
            pltpu.VMEM((heads, half, hd), jnp.bfloat16),
            pltpu.VMEM((heads, half, hd), jnp.bfloat16),
            pltpu.VMEM((heads, half, hd), jnp.bfloat16),
            pltpu.VMEM((m - 1, heads, half, hd), jnp.bfloat16),
            dma((nqc + 2,)), dma((nqc + 1,)), dma((nqc + 1,)),
            dma((m - 1, nqc + 1)), dma((m - 1, nqc + 1)), dma((nqc,)), dma((nqc,)),
        ],
        compiler_params=pltpu.CompilerParams(
            collective_id=0, has_side_effects=True, vmem_limit_bytes=VMEM_LIMIT),
    )(x, wq, wk, wv, cos, sin, ptt, lens)


def finish_kernel(
    m, ntp, o, stats, q, kv, wout, out,
    wbuf, r1o, r1s, mo, s2o, s2s, r2o, r2s, tile, ho, snew, tsend, kept, trecv,
    wsem, s1sem, r1sem, s2sem, r2sem, s3sem, r3sem, s4sem, r4sem,
):
    nq, half, hd = mo.shape
    nqp = stats.shape[1] // 2
    core, partner, peers = place(m)
    tp = lax.axis_index("tp")
    load = pltpu.make_async_copy(wout, wbuf, wsem)
    load.start()
    greet(
        [("kvp", partner)] + [("kvp", p) for p in peers]
        + [("tp", (tp + d) % ntp) for d in range(1, ntp)]
    )
    mine = pl.ds(pl.multiple_of(core * half, half), half)
    batch = o.shape[1]
    rows = batch // ntp
    parts = chunks_of(nq, 3)
    count = len(parts)
    chunks = steps_of(half, batch // ntp)
    size = half // chunks
    stat1 = remote(stats.at[1 - core], r1s, s1sem.at[0, count], r1sem.at[0, count], "kvp", partner)
    stat1.start()
    first = {}
    for r in range(chunks):
        theirs = pl.ds(pl.multiple_of((1 - core) * half + r * size, size), size)
        for i, (h0, n) in enumerate(parts):
            copy = remote(
                o.at[pl.ds(h0, n), theirs, :], r1o.at[pl.ds(h0, n), pl.ds(r * size, size), :],
                s1sem.at[r, i], r1sem.at[r, i], "kvp", partner)
            copy.start()
            first[r, i] = copy
    nkv = kv.shape[0] // 2
    group = nq // nkv
    ones = jnp.ones((8, hd), jnp.float32)
    snew[...] = jnp.full(snew.shape, NEG, jnp.float32)
    for h in range(nq):
        product = q[h, mine, :].astype(jnp.float32) * kv[h // group].astype(jnp.float32)
        row = lax.dot_general(
            ones, product, (((1,), (1,)), ((), ())),
            precision=lax.Precision.HIGHEST, preferred_element_type=jnp.float32)
        snew[h:h + 1, :] = row[0:1] * (hd ** -0.5)

    def merged(sources):
        top = sources[0][0]
        for t, _ in sources[1:]:
            top = jnp.maximum(top, t)
        raw = [jnp.exp(t - top) * total for t, total in sources]
        total = raw[0]
        for r in raw[1:]:
            total = total + r
        safe = jnp.where(total > 0.0, total, 1.0)
        for k, r in enumerate(raw):
            tile[k * nqp:(k + 1) * nqp, :] = r / safe
        return top, total, tile[...].T

    tile[...] = jnp.zeros(tile.shape, jnp.float32)
    stat1.wait_recv()
    top, total, cols = merged([
        (stats[core, :nqp], stats[core, nqp:]), (r1s[:nqp], r1s[nqp:]),
    ])
    s2s[:nqp] = top
    s2s[nqp:] = total
    stat2 = []
    for s, peer in enumerate(peers):
        copy = remote(s2s, r2s.at[s], s2sem.at[s, 0, count], r2sem.at[s, 0, count], "kvp", peer)
        copy.start()
        stat2.append(copy)
    second = {}
    for r in range(chunks):
        span = pl.ds(r * size, size)
        ours = pl.ds(pl.multiple_of(core * half + r * size, size), size)
        part_cols = cols[r * size:(r + 1) * size]
        for i, (h0, n) in enumerate(parts):
            first[r, i].wait_recv()
            for h in range(h0, h0 + n):
                value = (
                    part_cols[:, h:h + 1] * o[h, ours, :].astype(jnp.float32)
                    + part_cols[:, nqp + h:nqp + h + 1] * r1o[h, span, :].astype(jnp.float32)
                )
                mo[h, span, :] = value
                s2o[h, span, :] = value.astype(jnp.bfloat16)
            for s, peer in enumerate(peers):
                copy = remote(
                    s2o.at[pl.ds(h0, n), span, :], r2o.at[s, pl.ds(h0, n), span, :],
                    s2sem.at[s, r, i], r2sem.at[s, r, i], "kvp", peer)
                copy.start()
                second[s, r, i] = copy
    for copy in stat2:
        copy.wait_recv()
    sources = [(top, total)]
    for s in range(len(peers)):
        sources.append((r2s[s, :nqp], r2s[s, nqp:]))
    sources.append((snew[...], jnp.ones(snew.shape, jnp.float32)))
    _, _, cols = merged(sources)
    last = len(sources) - 1
    pieces, _, width = tsend.shape
    third = []

    def crossing(t, j):
        return remote(
            tsend.at[j, pl.ds(t * rows, rows), :], trecv.at[(tp - t + ntp) % ntp - 1, j],
            s4sem.at[t, j], r4sem.at[(tp - t + ntp) % ntp - 1, j], "tp", t)

    for r in range(chunks):
        span = pl.ds(r * size, size)
        part_cols = cols[r * size:(r + 1) * size]
        halves = []
        for i, (h0, n) in enumerate(parts):
            for s in range(len(peers)):
                second[s, r, i].wait_recv()
            for h in range(h0, h0 + n):
                value = part_cols[:, h:h + 1] * mo[h, span, :]
                for s in range(len(peers)):
                    at = (s + 1) * nqp + h
                    value = value + part_cols[:, at:at + 1] * r2o[s, h, span, :].astype(jnp.float32)
                at = last * nqp + h
                value = value + part_cols[:, at:at + 1] * kv[nkv + h // group, span, :].astype(jnp.float32)
                ho[core, span, h * hd:(h + 1) * hd] = value.astype(jnp.bfloat16)
            part = ho.at[core, span, pl.ds(h0 * hd, n * hd)]
            copy = remote(part, part, s3sem.at[r, i], r3sem.at[r, i], "kvp", partner)
            copy.start()
            halves.append(copy)
        third.extend(halves)
        if r == 0:
            load.wait()
        for copy in halves:
            copy.wait_recv()
        finished = jnp.concatenate([ho[0, span, :], ho[1, span, :]], axis=0)
        for j in range(pieces):
            terms = jnp.dot(
                finished, wbuf[:, j * width:(j + 1) * width], preferred_element_type=jnp.float32)
            for c in range(2):
                for k in range(size // rows):
                    t = (c * half + r * size) // rows + k
                    block = terms[c * size + k * rows:c * size + (k + 1) * rows]
                    tsend[j, t * rows:(t + 1) * rows, :] = block.astype(jnp.bfloat16)

                    @pl.when(t == tp)
                    def _():
                        kept[:, j * width:(j + 1) * width] = block

                    @pl.when(t != tp)
                    def _():
                        crossing(t, j).start()

    for j in range(pieces):
        value = kept[:, j * width:(j + 1) * width]
        for d in range(1, ntp):
            remote(
                tsend.at[j, pl.ds(0, rows), :], trecv.at[d - 1, j],
                s4sem.at[0, j], r4sem.at[d - 1, j], "tp", (tp + d) % ntp).wait_recv()
            value = value + trecv[d - 1, j].astype(jnp.float32)
        out[:, j * width:(j + 1) * width] = value.astype(jnp.bfloat16)
    stat1.wait_send()
    for copy in list(first.values()) + stat2 + list(second.values()) + third:
        copy.wait_send()
    for t in range(ntp):
        for j in range(pieces):

            @pl.when(t != tp)
            def _():
                crossing(t, j).wait_send()


def steps_of(half, rows):
    return 2 if (half // 2) % rows == 0 else 1


def finish(m, ntp, o, stats, q, kv, wout):
    nq, batch, hd = o.shape
    half = batch // 2
    nqp = stats.shape[1] // 2
    count = len(chunks_of(nq, 3))
    width = wout.shape[1]
    pieces = len(chunks_of(width // hd, 3))
    rows = batch // ntp
    tile_rows = max((m + 1) * nqp, half)
    chunks = steps_of(half, rows)
    vmem = pl.BlockSpec(memory_space=pltpu.VMEM)
    hbm = pl.BlockSpec(memory_space=pl.ANY)
    dma = pltpu.SemaphoreType.DMA
    return pl.pallas_call(
        functools.partial(finish_kernel, m, ntp),
        out_shape=jax.ShapeDtypeStruct((rows, width), jnp.bfloat16),
        in_specs=[vmem, vmem, vmem, vmem, hbm],
        out_specs=vmem,
        scratch_shapes=[
            pltpu.VMEM(wout.shape, jnp.bfloat16),
            pltpu.VMEM((nq, half, hd), jnp.bfloat16),
            pltpu.VMEM((2 * nqp, half), jnp.float32),
            pltpu.VMEM((nq, half, hd), jnp.float32),
            pltpu.VMEM((nq, half, hd), jnp.bfloat16),
            pltpu.VMEM((2 * nqp, half), jnp.float32),
            pltpu.VMEM((m - 1, nq, half, hd), jnp.bfloat16),
            pltpu.VMEM((m - 1, 2 * nqp, half), jnp.float32),
            pltpu.VMEM((tile_rows, half), jnp.float32),
            pltpu.VMEM((2, half, nq * hd), jnp.bfloat16),
            pltpu.VMEM((nqp, half), jnp.float32),
            pltpu.VMEM((pieces, batch, width // pieces), jnp.bfloat16),
            pltpu.VMEM((rows, width), jnp.float32),
            pltpu.VMEM((ntp - 1, pieces, rows, width // pieces), jnp.bfloat16),
            dma, dma((chunks, count + 1)), dma((chunks, count + 1)),
            dma((m - 1, chunks, count + 1)), dma((m - 1, chunks, count + 1)),
            dma((chunks, count)), dma((chunks, count)),
            dma((ntp, pieces)), dma((ntp - 1, pieces)),
        ],
        compiler_params=pltpu.CompilerParams(
            collective_id=1, has_side_effects=True, vmem_limit_bytes=VMEM_LIMIT),
    )(o, stats, q, kv, wout)


def attend(owned, valid, mt, key_cache, value_cache):
    nq, _, hd = owned.shape
    batch = mt.shape[1]
    nkv, slots, page, _ = key_cache.shape
    group = nq // nkv
    hit = mt >= 0
    mask = valid[None, :, None, :]
    owned = owned.reshape(nkv, group, slots, hd)
    scores = jnp.einsum(
        "hgpd,hptd->hpgt", owned, key_cache, preferred_element_type=jnp.float32) * hd ** -0.5
    scores = jnp.where(mask, scores, NEG)
    slot_top = jnp.max(scores, axis=-1)
    weights = jnp.where(mask, jnp.exp(scores - slot_top[..., None]), 0.0)
    slot_total = jnp.sum(weights, axis=-1)
    slot_acc = jnp.einsum(
        "hpgt,hptd->hpgd", weights.astype(jnp.bfloat16), value_cache,
        preferred_element_type=jnp.float32)
    cover = hit[None, :, None, :]
    top = jnp.max(jnp.where(cover, slot_top[..., None], NEG), axis=1)
    factor = jnp.where(cover, jnp.exp(slot_top[..., None] - top[:, None]), 0.0)
    total = jnp.sum(factor * slot_total[..., None], axis=1)
    acc = jnp.einsum("hpgb,hpgd->hgbd", factor, slot_acc, preferred_element_type=jnp.float32)
    safe = jnp.where(total > 0.0, total, 1.0)
    o = (acc / safe[..., None]).astype(jnp.bfloat16).reshape(nq, batch, hd)
    nqp = -(-nq // 8) * 8
    pad = ((0, nqp - nq), (0, 0))
    stats = jnp.concatenate(
        [
            jnp.pad(top.reshape(nq, batch), pad, constant_values=NEG),
            jnp.pad(total.reshape(nq, batch), pad),
        ]
    )
    return o, stats.reshape(2 * nqp, 2, batch // 2).transpose(1, 0, 2)


def body(m, ntp, normed, w_query, w_key, w_value, w_out, key_cache, value_cache, lengths, page_table):
    hd = key_cache.shape[3]
    cos, sin = angles(lengths.astype(jnp.float32), hd)
    q, kv, mt, owned, valid = project(
        m, normed, w_query, w_key, w_value, cos, sin, page_table.T, lengths[None, :],
        key_cache.shape[1], key_cache.shape[2], hd)
    o, stats = attend(owned, valid > 0, mt, key_cache, value_cache)
    return finish(m, ntp, o, stats, q, kv, w_out)


def solution(mesh):
    return jax.shard_map(
        functools.partial(body, mesh.shape["kvp"] // 2, mesh.shape["tp"]),
        mesh=mesh,
        in_specs=(
            P("grp", "kvp"),
            P("kvp", "tp"),
            P("kvp", "tp"),
            P("kvp", "tp"),
            P("tp", "kvp"),
            P("tp", ("grp", "kvp"), None, None),
            P("tp", ("grp", "kvp"), None, None),
            P("grp"),
            P("grp", None),
        ),
        out_specs=P(("grp", "tp"), "kvp"),
        check_vma=False,
    )
```
